256 devices in a mesh: tp: 8 (over z_lo, x), dp: 8 (over y, core), rep: 4 (over z_hi).
Axes of the slice: x: 4, y: 4, z: 8 (z_hi: 4, z_lo: 2; z = z_hi * 2 + z_lo), core: 2. Of those that a mesh axis runs over, the one named last changes fastest.
Arguments:
- prompts: bfloat16 [24576, 8192], P(('dp', 'rep'), 'tp'), may hold values from -6 to 6
- frozen_projection_weight: bfloat16 [2, 8192, 2048], P(None, ('dp', 'rep'), 'tp'), may hold values from -5 to 5
- lowrank_down_factor: bfloat16 [2, 8192, 64], P(None, ('dp', 'rep')), may hold values from -0.119628906 to 0.119628906
- lowrank_up_factor: bfloat16 [2, 64, 2048], P(None, None, 'tp'), may hold values from -0.59765625 to 0.59765625
- magnitude: float32 [2, 2048], P(None, 'tp'), may hold values from 0.5 to 2
Outputs:
- key_values: bfloat16 [2, 24576, 2048], P(None, ('dp', 'rep'), 'tp')
The draws below stay inside these ranges and needn't reach their ends.
All inputs are finite; a program needn't handle non-finite values.
Results may differ from the reference program's by a relative error of at most 0.0049.
Values may be sent and summed in bfloat16 or wider, within the bound.
No kernel may reach another device: no remote copies, remote signals or barrier semaphores. Data moves between devices by JAX's collectives and lax.ppermute only.
A program may use at most 64 MiB of HBM per device.

```python
import math
import jax
import jax.numpy as jnp
from jax import lax

MODEL_WIDTH = 8192
LOWRANK_SIZE = 64
LAYER_COUNT = 2
PROJECTION_COLUMNS = 2048
TOKENS = 24576


def draw_frozen_projection_weight(key, part):
    streams = jax.random.split(jax.random.fold_in(key, 17), 3)
    position = jnp.arange(MODEL_WIDTH, dtype=jnp.float32)[None, :, None] / MODEL_WIDTH
    row_rough = jnp.exp(jax.random.uniform(streams[1], (LAYER_COUNT, MODEL_WIDTH, 1), jnp.float32, -1.2, 1.2))
    col_rough = jnp.exp(jax.random.uniform(streams[2], (LAYER_COUNT, 1, PROJECTION_COLUMNS), jnp.float32, -1.2, 1.2))
    noise = jnp.clip(jax.random.normal(streams[0], (LAYER_COUNT, MODEL_WIDTH, PROJECTION_COLUMNS), jnp.float32), -4.0, 4.0)
    ramp = jnp.sqrt(1.0 + 2.0 * position)
    values = noise * row_rough * col_rough * ramp / math.sqrt(MODEL_WIDTH)
    return values.astype(jnp.bfloat16)


def steps_of(key, extent, cuts, low, top_value):
    gain = 1.0
    for dim, shards_of in cuts:
        draws = jax.random.uniform(jax.random.fold_in(jax.random.fold_in(key, 6), dim), (shards_of,), jnp.float32, low / len(cuts), top_value / len(cuts))
        gain = gain * jnp.repeat(jnp.exp(draws), extent[dim] // shards_of).reshape((-1,) + (1,) * (len(extent) - 1 - dim))
    return gain


def gaussian(rng, shape, deviation, reach, shards=(), held_as=jnp.bfloat16):
    values = jax.random.normal(rng, shape, jnp.float32) * deviation
    if len(shards) > 0:
        values = steps_of(rng, shape, shards, -0.22, 0.18) * values
    return jnp.clip(values, min=-reach, max=reach).astype(held_as)


def setup_inputs(seed: int = 0) -> dict:
    keys = jax.random.split(jax.random.key(seed), 6)
    return {
        "prompts": gaussian(keys[0], (TOKENS, MODEL_WIDTH), 1.0, 6.0, ((0, 32), (1, 8))),
        "frozen_projection_weight": draw_frozen_projection_weight(jax.random.fold_in(keys[5], 71), 0),
        "lowrank_down_factor": gaussian(keys[2], (LAYER_COUNT, MODEL_WIDTH, LOWRANK_SIZE), 0.02, 0.119628906, ((1, 32),)),
        "lowrank_up_factor": gaussian(keys[3], (LAYER_COUNT, LOWRANK_SIZE, PROJECTION_COLUMNS), 0.1, 0.59765625, ((2, 8),)),
        "magnitude": jnp.clip(jnp.exp(math.log(2.0) - 1.3862944 * jax.random.uniform(keys[4], (LAYER_COUNT, PROJECTION_COLUMNS), jnp.float32) ** steps_of(keys[4], (LAYER_COUNT, PROJECTION_COLUMNS), ((1, 8),), -0.2, 0.2)), 0.5, 2.0),
    }


epsilon = 1e-06

def reference(prompts, frozen_projection_weight, lowrank_down_factor, lowrank_up_factor, magnitude):
    outputs = []
    for current_layer_index in range(LAYER_COUNT):
        combined_weight = frozen_projection_weight[current_layer_index].astype(jnp.float32) + jnp.dot(lowrank_down_factor[current_layer_index], lowrank_up_factor[current_layer_index], preferred_element_type=jnp.float32)
        norms = jnp.sqrt(lax.optimization_barrier(jnp.sum(combined_weight * combined_weight, axis=0)) + epsilon)
        factor = magnitude[current_layer_index] / norms
        prefilled_key_values = (combined_weight * factor).astype(jnp.bfloat16)
        outputs.append(jnp.dot(prompts, prefilled_key_values, preferred_element_type=jnp.float32).astype(jnp.bfloat16))
    return jnp.stack(outputs)
```

```python
import jax
import jax.numpy as jnp
from jax import lax
from jax.experimental import pallas as pl
from jax.experimental.pallas import tpu as pltpu
from jax.sharding import Mesh
from jax.sharding import PartitionSpec as P


AXES = ("zl", "x", "y", "c", "zh")
EPSILON = 1e-06
F32 = jnp.float32
BF16 = jnp.bfloat16
CHUNKS = 2


def shift(value, axis, by):
    n = lax.axis_size(axis)
    return lax.ppermute(value, axis, [(i, (i + by) % n) for i in range(n)])


def transpose_rows(value):
    pairs = []
    for zl in range(2):
        for y in range(4):
            to = (zl, y) if y // 2 == zl else (1 - zl, 3 - y)
            pairs.append((zl * 4 + y, to[0] * 4 + to[1]))
    return lax.ppermute(value, ("zl", "y"), pairs)


ZH_OFFSETS = (0, 3, 1, 2)


def product_kernel(n_weights, weight_keys, with_squares, *refs):
    x_refs = refs[:4]
    w_refs = refs[4 : 4 + n_weights]
    outs = refs[4 + n_weights :]
    own_ref, send_ref = outs[:2]
    squares_ref = outs[2] if with_squares else None
    xs, acc = outs[-2:]
    zl, x, y, c, zh = (lax.axis_index(a) for a in AXES)
    for k, offset in enumerate(ZH_OFFSETS):
        start = pl.multiple_of(lax.rem(zh + offset, 4) * 256, 256)
        for j in range(4):
            xs[j, :, pl.ds(k * 256, 256)] = x_refs[j][:, pl.ds(start, 256)]
    acc[...] = jnp.zeros_like(acc)
    if with_squares:
        squares_ref[...] = jnp.zeros_like(squares_ref)
    for (r, other, k0, nk), w_ref in zip(weight_keys, w_refs, strict=True):
        y_from = lax.rem(y + r, 4)
        stayed = y_from // 2 == zl
        odd = lax.rem(y_from, 2)
        c_from = 1 - c if other else c
        feature_block = 2 * jnp.where(stayed, odd, 1 - odd) + c_from
        j = lax.rem(feature_block - x + 4, 4)
        side = jnp.where(stayed, 0, 1)
        for layer in range(2):
            w = w_ref[layer].reshape(nk * 256, 256)
            acc[side, layer] += jnp.dot(
                xs[j, :, k0 * 256 : (k0 + nk) * 256], w, preferred_element_type=F32
            )
            if with_squares:
                wide = w.astype(F32)
                squares_ref[side, layer] += jnp.sum(
                    (wide * wide).reshape(nk * 32, 8, 256), axis=0
                )
    own_ref[...] = acc[0]
    send_ref[...] = acc[1].astype(BF16)


def products(xs, weights, with_squares):
    tokens = xs[0].shape[0]
    keys = tuple(weights)
    out_shape = [
        jax.ShapeDtypeStruct((2, tokens, 256), F32),
        jax.ShapeDtypeStruct((2, tokens, 256), BF16),
    ]
    if with_squares:
        out_shape.append(jax.ShapeDtypeStruct((2, 2, 8, 256), F32))
    vmem = pl.BlockSpec(memory_space=pltpu.VMEM)
    return pl.pallas_call(
        lambda *refs: product_kernel(len(keys), keys, with_squares, *refs),
        out_shape=out_shape,
        in_specs=[vmem] * (4 + len(keys)),
        out_specs=[vmem] * len(out_shape),
        scratch_shapes=[
            pltpu.VMEM((4, tokens, 1024), BF16),
            pltpu.VMEM((2, 2, tokens, 256), F32),
        ],
        cost_estimate=pl.CostEstimate(
            flops=2 * tokens * 4096 * 1024, bytes_accessed=16 << 20, transcendentals=0
        ),
        name="products",
    )(*xs, *weights.values())


def local(prompts, frozen, down, up, magnitude):
    tokens = prompts.shape[0] // CHUNKS
    chunks = [prompts[q * tokens : (q + 1) * tokens] for q in range(CHUNKS)]
    gathered = []
    for q, chunk in enumerate(chunks):
        from_left = shift(chunk, "x", 1)
        from_right = shift(chunk, "x", -1)
        far = shift(from_left, "x", 1) if q % 2 == 0 else shift(from_right, "x", -1)
        gathered.append([chunk, from_right, far, from_left])

    merged = frozen.astype(F32) + jnp.einsum("lir,lrj->lij", down, up, preferred_element_type=F32)
    first = transpose_rows(merged.astype(BF16))
    rest = jnp.stack(
        [shift(first, "zh", 1), shift(first, "zh", -1), shift(first, "zh", 2)], axis=1
    )
    first = first[:, None]
    near = {0: [(0, 1, first), (1, 3, rest)]}
    near[3] = [(0, 1, shift(first, "y", 1)), (1, 3, shift(rest, "y", 1))]
    near[1] = [(0, 1, shift(first, "y", -1)), (1, 3, shift(rest, "y", -1))]
    near[2] = [
        (0, 1, shift(near[3][0][2], "y", 1)),
        (1, 1, shift(near[3][1][2][:, :1], "y", 1)),
        (2, 2, shift(near[1][1][2][:, 1:], "y", -1)),
    ]
    weights = {}
    for r, pieces in near.items():
        for k0, nk, piece in pieces:
            weights[r, False, k0, nk] = piece
            weights[r, True, k0, nk] = shift(piece, "c", 1)

    results = []
    scale = None
    for q in range(CHUNKS):
        own, send, *squares = products(gathered[q], weights, q == 0)
        got = shift(send, "zl", 1)
        if squares:
            sums = jnp.sum(squares[0], axis=2)
            sums = sums[0] + shift(sums[1], "zl", 1)
            scale = magnitude / jnp.sqrt(sums + EPSILON)
        results.append(((own + got.astype(F32)) * scale[:, None, :]).astype(BF16))
    return jnp.concatenate(results, axis=1)


def solution(mesh):
    split = Mesh(mesh.devices.reshape(2, 4, 4, 2, 4), AXES)
    rows, columns = ("y", "c", "zh"), ("zl", "x")
    in_specs = (
        P(rows, columns),
        P(None, rows, columns),
        P(None, rows, None),
        P(None, None, columns),
        P(None, columns),
    )
    return jax.shard_map(
        local, mesh=split, in_specs=in_specs, out_specs=P(None, rows, columns), check_vma=False
    )
```
